512 devices in a mesh: groups: 2 (over y), ep: 32 (over z, core), tp: 8 (over x).
Axes of the slice: x: 8, y: 2, z: 16, core: 2. Of those that a mesh axis runs over, the one named last changes fastest.
The devices are a block of a 8x8x16 slice.
Arguments:
- context: bfloat16 [4096, 4096], P(('groups', 'ep'), 'tp'), parts along dimension 0, may hold values from -6 to 6
- stream: bfloat16 [4096, 4096], P(('groups', 'ep'), 'tp'), parts along dimension 0, may hold values from -14 to 14
- out_proj: bfloat16 [4096, 4096], P('tp', 'ep'), may hold values from -0.09375 to 0.09375
- norm_gain: bfloat16 [4096], P('tp'), may hold values from 0.099609375 to 1.8984375
- router: bfloat16 [4096, 4], P('tp'), may hold values from -0.0625 to 0.0625
- expert_ids: int32 [4096, 2], P(('groups', 'ep')), parts along dimension 0, may hold values from 0 to 3, all different within a row; in each aligned block of 64 rows (0 to 63, 64 to 127, ...) at most 36 rows name the same one
- w_gate: bfloat16 [4096, 28672], P('tp', 'ep'), may hold values from -0.09375 to 0.09375
- w_up: bfloat16 [4096, 28672], P('tp', 'ep'), may hold values from -0.09375 to 0.09375
- w_down: bfloat16 [28672, 4096], P('ep', 'tp'), may hold values from -0.125 to 0.125
Outputs:
- layer_out: bfloat16 [4096, 4096], P(('groups', 'ep'), 'tp'), parts along dimension 0
The draws below stay inside these ranges and needn't reach their ends.
There are 2 independent parts, one for each index of `groups`. The reference program is written for one: setup_inputs(seed, part) draws one part's arguments, and reference() takes and returns one part's arrays. A program takes and returns all parts, laid end to end along the dimension named above; an argument that names none is the same for every part. Nothing has to cross between parts.
Inputs may be any that keep to these rules, and one draw needn't show every extreme that they name: `expert_ids`: each row names 2 different experts. In each aligned block of 64 rows (the rows of one index of ep) no expert is named by more than 36 rows, and in some blocks one expert is named by exactly 36 rows.
All inputs are finite; a program needn't handle non-finite values.
Results may differ from the reference program's by a relative error of at most 0.02.
Values may be sent and summed in bfloat16 or wider, within the bound.
No kernel may reach another device: no remote copies, remote signals or barrier semaphores. Data moves between devices by JAX's collectives and lax.ppermute only.
A program may use at most 64 MiB of HBM per device.

```python
import math
import jax
import jax.numpy as jnp
import numpy as np
from jax import lax

D = 4096
EXPERTS = 4
TOP = 2
FF = 7168
TOK = 64
ATT = 4096
CAP = 36
TOKENS = 2048
N_EP = 32
N_TP = 8


def draw_stream(key, part):
    key_base, key_rows = jax.random.split(jax.random.fold_in(key, 17))
    col_scale = jnp.exp(jnp.log(3.0) * jnp.arange(D, dtype=jnp.float32) / D) / jnp.sqrt(3.0)
    noise_base = jax.random.truncated_normal(key_base, -4.0, 4.0, (TOKENS, D), jnp.float32)
    row_scale = jnp.exp(jax.random.uniform(key_rows, (TOKENS, 1), jnp.float32, jnp.log(0.2), jnp.log(2.0)))
    return (noise_base * row_scale * col_scale[None, :]).astype(jnp.bfloat16)


def shard_levels(key, dims, cuts, low, high):
    loudness, own = 1.0, jax.random.fold_in(key, 6)
    for axis_at, blocks in cuts:
        heights = jnp.exp(jax.random.uniform(jax.random.fold_in(own, axis_at), (blocks,), jnp.float32, low / len(cuts), high / len(cuts)))
        loudness = loudness * jnp.repeat(heights, dims[axis_at] // blocks).reshape([-1 if axis == axis_at else 1 for axis in range(len(dims))])
    return loudness


def assign_block(key, own, number, rows, number_of, top, most, lean):
    sequence = jax.random.permutation(key, number_of)
    heavy_load, common = shares(number_of, rows * top, most, lean, True), shares(number_of, rows * top, most, lean, False)
    places = jnp.arange(number_of)

    def named(tallies, turn):
        used = int((tallies > 0).sum())
        fixed = max(1, used // 4)
        moved = fixed + (places - fixed + turn * (used - fixed)) % max(1, number_of - fixed)
        return jnp.zeros((number_of,), jnp.int32).at[sequence[jnp.where(places < fixed, places, moved)]].set(jnp.asarray(tallies, jnp.int32))

    tallies = jnp.where(number % 4 == 0, named(heavy_load, number // 4), named(common, number - number // 4 - 1))
    mixed = jax.random.permutation(jax.random.fold_in(own, 3), number_of)
    donor, receiver = mixed[0:number_of // 2 * 2:2], mixed[1:number_of // 2 * 2:2]
    room = jnp.minimum(tallies[donor] - 1, most - tallies[receiver]) // 2
    room = jnp.where((donor == sequence[0]) | (receiver == sequence[0]) | (tallies[receiver] == 0), 0, jnp.maximum(room, 0))
    moved = jax.random.randint(jax.random.fold_in(own, 4), (number_of // 2,), 0, 1 << 20) % (room + 1)
    tallies = tallies.at[donor].add(-moved).at[receiver].add(moved)
    members = jnp.searchsorted(jnp.cumsum(tallies), jnp.arange(rows * top), side="right").astype(jnp.int32)
    listing = members.reshape(top, rows).T
    listing = listing[jax.random.permutation(jax.random.fold_in(own, 1), rows)]
    turn = jax.random.randint(jax.random.fold_in(own, 2), (rows, 1), 0, top)
    return jnp.take_along_axis(listing, (jnp.arange(top)[None, :] + turn) % top, axis=1)


def shares(number_of, total, most, lean, full):
    loads = [(1 << 20) // math.isqrt(rank ** lean) + 1 for rank in range(1, number_of + 1)]
    largest = most if full else min(most, max(-(-total // number_of), total * loads[0] // sum(loads)))
    least = 1 if total - largest >= number_of - 1 else 0
    given, surplus = [largest] + [least] * (number_of - 1), total - largest - least * (number_of - 1)
    while surplus > 0:
        free = [i for i in range(1, number_of) if given[i] < largest] or [i for i in range(1, number_of) if given[i] < most]
        pool, remaining = sum([loads[i] for i in free]), surplus
        for i in free:
            extra = min(most - given[i], max(1, remaining * loads[i] // pool), surplus)
            given[i] = given[i] + extra
            surplus = surplus - extra
    return np.array(given)


def centred(rng, dims, deviation, limit, cuts=(), kind=jnp.bfloat16):
    level = shard_levels(rng, dims, cuts, -0.22, 0.18) if cuts else 1.0
    array = jax.random.normal(rng, dims, jnp.float32) * deviation * level
    return jnp.minimum(jnp.maximum(array, -limit), limit).astype(kind)


def setup_inputs(seed: int = 0, part: int = 0) -> dict:
    splits = jax.random.split(jax.random.key(seed), 10)
    part_keys = jax.random.split(jax.random.fold_in(splits[9], part), 10)
    context = centred(part_keys[0], (TOKENS, ATT), 1.0, 6.0, ((0, 32), (1, 8)))
    stream = draw_stream(jax.random.fold_in(jax.random.fold_in(splits[9], part), 71), part)
    out_proj = centred(splits[2], (ATT, D), ATT ** -0.5, 0.09375, ((0, 8), (1, 32)))
    norm_gain = jnp.clip(1.0 + 0.18 * jax.random.normal(splits[3], (D,), jnp.float32), 0.099609375, 1.8984375).astype(jnp.bfloat16)
    router = centred(splits[4], (D, EXPERTS), (2 * D) ** -0.5, 0.0625, ((0, 8),))
    expert_ids_keys = jax.random.split(jax.random.fold_in(part_keys[5], 1), TOKENS // TOK)
    expert_ids_turns = jax.random.permutation(jax.random.fold_in(part_keys[5], 3), TOKENS // TOK)
    expert_ids = jax.vmap(lambda own, number: assign_block(jax.random.fold_in(part_keys[5], 2), own, number, TOK, EXPERTS, TOP, CAP, 2))(expert_ids_keys, expert_ids_turns).reshape((TOKENS, TOP))
    w_gate = centred(splits[6], (D, EXPERTS * FF), D ** -0.5, 0.09375, ((0, 8), (1, 32)))
    w_up = centred(splits[7], (D, EXPERTS * FF), D ** -0.5, 0.09375, ((0, 8), (1, 32)))
    w_down = centred(splits[8], (EXPERTS * FF, D), (FF // 4) ** -0.5, 0.125, ((0, 32), (1, 8)))
    return {"context": context, "stream": stream, "out_proj": out_proj, "norm_gain": norm_gain, "router": router, "expert_ids": expert_ids, "w_gate": w_gate, "w_up": w_up, "w_down": w_down}


def rounded(tensor):
    return lax.optimization_barrier(tensor.astype(jnp.bfloat16)).astype(jnp.float32)

def reference(context, stream, out_proj, norm_gain, router, expert_ids, w_gate, w_up, w_down):
    head_cols = ATT // N_TP
    attention = jnp.zeros((TOKENS, D), jnp.float32)
    for device_lane in range(N_TP):
        low_index = device_lane * head_cols
        attention = attention + rounded(jnp.dot(context[:, low_index:low_index + head_cols], out_proj[low_index:low_index + head_cols], preferred_element_type=jnp.float32))
    hstate = (stream.astype(jnp.float32) + attention).astype(jnp.bfloat16)
    hfloat = hstate.astype(jnp.float32)
    inverse = lax.rsqrt(lax.optimization_barrier(jnp.mean(hfloat * hfloat, axis=1, keepdims=True)) + 1e-05)
    normed = hfloat * inverse * norm_gain.astype(jnp.float32)
    logits = jnp.dot(normed, router.astype(jnp.float32), precision=lax.Precision.HIGHEST)
    inputs = normed.astype(jnp.bfloat16)
    experts_range = jnp.arange(EXPERTS, dtype=jnp.int32)
    picked = expert_ids[:, :, None] == experts_range[None, None, :]
    chosen = lax.optimization_barrier(jnp.sum(jnp.where(picked, logits[:, None, :], jnp.zeros_like(logits[:, None, :])), axis=2))
    leading = jax.nn.sigmoid(chosen[:, 0] - chosen[:, 1])
    weights = jnp.stack([leading, 1.0 - leading], axis=1)
    flat_ids = expert_ids.reshape(N_EP, TOK * TOP)
    onehot = (flat_ids[:, :, None] == experts_range[None, None, :]).astype(jnp.int32)
    before = jnp.cumsum(onehot, axis=1) - onehot
    slot_index = lax.optimization_barrier(jnp.sum(before * onehot, axis=2))
    block_ids = jnp.arange(N_EP, dtype=jnp.int32)[:, None]
    target = ((flat_ids * N_EP + block_ids) * CAP + slot_index).reshape(TOKENS * TOP).astype(jnp.int32)
    owner_idx = (jnp.arange(TOKENS * TOP, dtype=jnp.int32) // TOP).astype(jnp.int32)
    slot_table = jnp.full((EXPERTS * N_EP * CAP,), TOKENS, jnp.int32).at[target].set(owner_idx)
    padded = jnp.concatenate([inputs, jnp.zeros((1, D), jnp.bfloat16)], axis=0)
    rows_all = padded[slot_table].reshape(EXPERTS, N_EP * CAP, D)
    part_rows = D // N_TP
    group_size = N_EP // EXPERTS
    block_size = FF // group_size
    outputs = []
    for expert in range(EXPERTS):
        chosen_rows = rows_all[expert]
        col_base = expert * FF
        gate_sum = jnp.zeros((N_EP * CAP, FF), jnp.float32)
        up_sum = jnp.zeros((N_EP * CAP, FF), jnp.float32)
        for device_lane in range(N_TP):
            low_index = device_lane * part_rows
            row_slice = chosen_rows[:, low_index:low_index + part_rows]
            gate_sum = gate_sum + rounded(jnp.dot(row_slice, w_gate[low_index:low_index + part_rows, col_base:col_base + FF], preferred_element_type=jnp.float32))
            up_sum = up_sum + rounded(jnp.dot(row_slice, w_up[low_index:low_index + part_rows, col_base:col_base + FF], preferred_element_type=jnp.float32))
        hidden = (jax.nn.silu(gate_sum) * up_sum).astype(jnp.bfloat16)
        expert_sum = jnp.zeros((N_EP * CAP, D), jnp.float32)
        for block_id in range(group_size):
            low_index = block_id * block_size
            expert_sum = expert_sum + rounded(jnp.dot(hidden[:, low_index:low_index + block_size], w_down[col_base + low_index:col_base + low_index + block_size], preferred_element_type=jnp.float32))
        outputs.append(expert_sum)
    expert_out = jnp.concatenate(outputs, axis=0)
    gathered = expert_out[target].reshape(TOKENS, TOP, D)
    expert_mix = lax.optimization_barrier(jnp.sum(gathered * weights[:, :, None], axis=1))
    return (hfloat + expert_mix).astype(jnp.bfloat16)
```

```python
import jax
import jax.numpy as jnp
from jax import lax
from jax.sharding import Mesh, PartitionSpec as P

D = 4096
EXPERTS = 4
CAP = 36
CORES = 2
EP = ("a", "q", "core")


def per_device(context, stream, out_proj, norm_gain, router, expert_ids, w_gate, w_up, w_down):
    f32, bf16 = jnp.float32, jnp.bfloat16
    tok_rows, width = stream.shape
    tp = lax.axis_size("tp")
    quads = lax.axis_size("q")
    swap = [(0, 1), (1, 0)]

    w_both = lax.optimization_barrier(jnp.concatenate([w_gate, w_up], axis=1))

    head_part = jnp.dot(
        context, lax.all_gather(out_proj, EP, axis=1, tiled=True), preferred_element_type=f32
    ).astype(bf16)
    cut = jnp.moveaxis(head_part.reshape(tok_rows, tp, width), 1, 0)
    parts = lax.all_to_all(cut, "tp", 0, 0, tiled=True)
    hstate = (stream.astype(f32) + jnp.sum(parts.astype(f32), axis=0)).astype(bf16)
    hfloat = hstate.astype(f32)
    gain = norm_gain.astype(f32)

    experts_range = jnp.arange(EXPERTS, dtype=jnp.int32)
    flat_ids = expert_ids.reshape(tok_rows * 2)
    onehot = (flat_ids[:, None] == experts_range[None, :]).astype(jnp.int32)
    before = jnp.cumsum(onehot, axis=0) - onehot
    target = flat_ids * CAP + jnp.sum(before * onehot, axis=1)
    columns_all = jnp.arange(EXPERTS * CAP, dtype=jnp.int32)
    placement = (
        (target[:, None] == columns_all[None, :]).astype(f32).reshape(tok_rows, 2, EXPERTS * CAP)
    )
    dispatch = jnp.sum(placement, axis=1).astype(bf16)
    sectioned = lax.dot_general(
        dispatch, hstate, (((0,), (0,)), ((), ())), preferred_element_type=f32
    ).astype(bf16)

    mine = lax.all_to_all(sectioned.reshape(EXPERTS, CAP, width), "a", 0, 0, tiled=True)
    chunk = EXPERTS * CAP
    chip = lax.all_gather(mine.reshape(chunk, width), "q", axis=0, tiled=True)
    other = lax.ppermute(chip, "core", swap)
    rows = jnp.concatenate([chip, other], axis=0)

    rfloat = rows.astype(f32)
    scaled = (rfloat * gain[None, :]).astype(bf16)
    row_sq = jnp.sum(rfloat * rfloat, axis=1)
    both = jnp.dot(scaled, w_both, preferred_element_type=f32).astype(bf16)
    squares = jnp.sum(hfloat * hfloat, axis=1)
    unscaled = jnp.dot(
        hfloat * gain[None, :], router.astype(f32), precision=lax.Precision.HIGHEST
    )
    both, row_sq, squares, unscaled = lax.optimization_barrier((both, row_sq, squares, unscaled))
    share = lax.psum_scatter(both, "tp", scatter_dimension=0, tiled=True).astype(f32)
    row_total, total_sq, raw_logits = lax.psum((row_sq, squares, unscaled), "tp")
    my_total = lax.dynamic_slice_in_dim(row_total, lax.axis_index("tp") * chunk, chunk)
    row_inverse = lax.rsqrt(my_total / D + 1e-05)[:, None]
    ff = w_gate.shape[1]
    gate_share, up_share = share[:, :ff] * row_inverse, share[:, ff:] * row_inverse
    hidden_share = (jax.nn.silu(gate_share) * up_share).astype(bf16)
    hidden = lax.all_gather(hidden_share, "tp", axis=0, tiled=True)
    partial_value = jnp.dot(hidden, w_down, preferred_element_type=f32).astype(bf16)

    half = quads * chunk
    from_core = lax.ppermute(partial_value[half:], "core", swap)
    on_chip = (partial_value[:half].astype(f32) + from_core.astype(f32)).astype(bf16)
    from_chips = lax.all_to_all(on_chip.reshape(quads, chunk, width), "q", 0, 0, tiled=True)
    summed = jnp.sum(from_chips.astype(f32), axis=0).astype(bf16)
    back = lax.all_to_all(summed.reshape(EXPERTS, CAP, width), "a", 0, 0, tiled=True)

    inverse = lax.rsqrt(total_sq / D + 1e-05)[:, None]
    logits = raw_logits * inverse
    picked = onehot.reshape(tok_rows, 2, EXPERTS).astype(f32)
    chosen = jnp.sum(picked * logits[:, None, :], axis=2)
    leading = jax.nn.sigmoid(chosen[:, 0] - chosen[:, 1])
    weights = jnp.stack([leading, 1.0 - leading], axis=1)
    combine = jnp.sum(placement * weights[:, :, None], axis=1)
    expert_mix = jnp.dot(
        combine, back.reshape(chunk, width).astype(f32), precision=lax.Precision.HIGHEST
    )
    return (hfloat + expert_mix).astype(bf16)


def solution(mesh):
    groups, ep, tp = (mesh.shape[name] for name in ("groups", "ep", "tp"))
    fine = Mesh(
        mesh.devices.reshape(groups, EXPERTS, ep // (EXPERTS * CORES), CORES, tp),
        ("groups", *EP, "tp"),
    )
    rows = ("groups", *EP)
    return jax.shard_map(
        per_device,
        mesh=fine,
        in_specs=(
            P(rows, "tp"),
            P(rows, "tp"),
            P("tp", EP),
            P("tp"),
            P("tp", None),
            P(rows, None),
            P("tp", EP),
            P("tp", EP),
            P(EP, "tp"),
        ),
        out_specs=P(rows, "tp"),
        check_vma=False,
    )
```

```python
import jax
import jax.numpy as jnp
from jax import lax
from jax.sharding import Mesh, PartitionSpec as P

D = 4096
EXPERTS = 4
CAP = 36
CORES = 2
EP = ("a", "q", "core")


def per_device(context, stream, out_proj, norm_gain, router, expert_ids, w_gate, w_up, w_down):
    f32, bf16 = jnp.float32, jnp.bfloat16
    tok_rows, width = stream.shape
    tp = lax.axis_size("tp")
    quads = lax.axis_size("q")
    swap = [(0, 1), (1, 0)]

    w_both = lax.optimization_barrier(jnp.concatenate([w_gate, w_up], axis=1))

    experts_range = jnp.arange(EXPERTS, dtype=jnp.int32)
    flat_ids = expert_ids.reshape(tok_rows * 2)
    onehot = (flat_ids[:, None] == experts_range[None, :]).astype(jnp.int32)
    before = jnp.cumsum(onehot, axis=0) - onehot
    target = flat_ids * CAP + jnp.sum(before * onehot, axis=1)
    columns_all = jnp.arange(EXPERTS * CAP, dtype=jnp.int32)
    placement = (
        (target[:, None] == columns_all[None, :]).astype(f32).reshape(tok_rows, 2, EXPERTS * CAP)
    )
    dispatch = jnp.sum(placement, axis=1).astype(bf16)
    proj_all = lax.all_gather(out_proj, EP, axis=1, tiled=True)
    proj_all, w_down, dispatch, placement, onehot = lax.optimization_barrier(
        (proj_all, w_down, dispatch, placement, onehot)
    )
    down_all = lax.all_gather(w_down, "tp", axis=0)
    head_part = jnp.dot(context, proj_all, preferred_element_type=f32).astype(bf16)
    cut = jnp.moveaxis(head_part.reshape(tok_rows, tp, width), 1, 0)
    parts = lax.all_to_all(cut, "tp", 0, 0, tiled=True)
    hstate = (stream.astype(f32) + jnp.sum(parts.astype(f32), axis=0)).astype(bf16)
    hfloat = hstate.astype(f32)
    gain = norm_gain.astype(f32)

    sectioned = lax.dot_general(
        dispatch, hstate, (((0,), (0,)), ((), ())), preferred_element_type=f32
    ).astype(bf16)

    mine = lax.all_to_all(sectioned.reshape(EXPERTS, CAP, width), "a", 0, 0, tiled=True)
    chunk = EXPERTS * CAP
    chip = lax.all_gather(mine.reshape(chunk, width), "q", axis=0, tiled=True)
    other = lax.ppermute(chip, "core", swap)
    first = lax.axis_index("core") == 0
    rows = jnp.concatenate([jnp.where(first, chip, other), jnp.where(first, other, chip)], axis=0)

    rfloat = rows.astype(f32)
    scaled = (rfloat * gain[None, :]).astype(bf16)
    row_sq = jnp.sum(rfloat * rfloat, axis=1)
    both = jnp.dot(scaled, w_both, preferred_element_type=f32).astype(bf16)
    squares = jnp.sum(hfloat * hfloat, axis=1)
    unscaled = jnp.dot(
        hfloat * gain[None, :], router.astype(f32), precision=lax.Precision.HIGHEST
    )
    both, down_all, row_sq, squares, unscaled = lax.optimization_barrier(
        (both, down_all, row_sq, squares, unscaled)
    )
    share = lax.psum_scatter(both, "tp", scatter_dimension=0, tiled=True)
    row_total, total_sq, raw_logits = lax.psum((row_sq, squares, unscaled), "tp")
    my_total = lax.dynamic_slice_in_dim(row_total, lax.axis_index("tp") * chunk, chunk)
    row_inverse = lax.rsqrt(my_total / D + 1e-05)[:, None]
    inverse = lax.rsqrt(total_sq / D + 1e-05)[:, None]
    logits = raw_logits * inverse
    picked = onehot.reshape(tok_rows, 2, EXPERTS).astype(f32)
    chosen = jnp.sum(picked * logits[:, None, :], axis=2)
    leading = jax.nn.sigmoid(chosen[:, 0] - chosen[:, 1])
    weights = jnp.stack([leading, 1.0 - leading], axis=1)
    combine = jnp.sum(placement * weights[:, :, None], axis=1)
    where = lax.axis_index("a")
    picks = [(where + step) % EXPERTS for step in range(EXPERTS)]
    mixed = combine.reshape(tok_rows, EXPERTS, CAP)
    by_step = [
        lax.dynamic_index_in_dim(mixed, (where - step) % EXPERTS, 1, keepdims=False)
        for step in range(EXPERTS)
    ]
    share, row_inverse, picks, by_step = lax.optimization_barrier(
        (share, row_inverse, picks, by_step)
    )
    ff = w_gate.shape[1]
    wide = share.astype(f32)
    gate_share, up_share = wide[:, :ff] * row_inverse, wide[:, ff:] * row_inverse
    hidden = (jax.nn.silu(gate_share) * up_share).astype(bf16)
    partial_value = jnp.stack(
        [
            jnp.dot(hidden, down_all[f], preferred_element_type=f32).astype(bf16)
            for f in range(tp)
        ]
    )

    halves = partial_value.reshape(CORES, quads, chunk, width)
    from_core = lax.all_to_all(halves, "core", 0, 0, tiled=True)
    on_chip = jnp.sum(from_core.astype(f32), axis=0).astype(bf16)
    from_chips = lax.all_to_all(on_chip, "q", 0, 0, tiled=True)
    summed = jnp.sum(from_chips.astype(f32), axis=0).astype(bf16).reshape(EXPERTS, CAP, width)

    sends = []
    for step in range(EXPERTS):
        pairs = []
        for e in range(EXPERTS):
            for q in range(quads):
                for c in range(CORES):
                    for t in range(tp):
                        dest = ((e + step) % EXPERTS, t % quads, t // quads, c * quads + q)
                        pairs.append((flat(quads, tp, e, q, c, t), flat(quads, tp, *dest)))
        piece = lax.dynamic_index_in_dim(summed, picks[step], 0, keepdims=False)
        sends.append(lax.ppermute(piece, (*EP, "tp"), pairs))
    expert_mix = sum(
        jnp.dot(weight, piece.astype(f32), precision=lax.Precision.HIGHEST)
        for weight, piece in zip(by_step, sends, strict=True)
    )
    return (hfloat + expert_mix).astype(bf16)


def flat(quads, tp, a, q, core, t):
    return ((a * quads + q) * CORES + core) * tp + t


def solution(mesh):
    groups, ep, tp = (mesh.shape[name] for name in ("groups", "ep", "tp"))
    fine = Mesh(
        mesh.devices.reshape(groups, EXPERTS, ep // (EXPERTS * CORES), CORES, tp),
        ("groups", *EP, "tp"),
    )
    rows = ("groups", *EP)
    return jax.shard_map(
        per_device,
        mesh=fine,
        in_specs=(
            P(rows, "tp"),
            P(rows, "tp"),
            P("tp", EP),
            P("tp"),
            P("tp", None),
            P(rows, None),
            P("tp", EP),
            P("tp", EP),
            P(EP, "tp"),
        ),
        out_specs=P(rows, "tp"),
        check_vma=False,
    )
```

```python
import jax
import jax.numpy as jnp
from jax import lax
from jax.sharding import Mesh, PartitionSpec as P

D = 4096
EXPERTS = 4
CAP = 36
CORES = 2
EP = ("a", "q", "core")
GROUP = ("q", "core")


def per_device(context, stream, out_proj, norm_gain, router, expert_ids, w_gate, w_up, w_down):
    f32, bf16 = jnp.float32, jnp.bfloat16
    tok_rows, width = stream.shape
    tp = lax.axis_size("tp")
    quads = lax.axis_size("q")
    swap = [(0, 1), (1, 0)]

    w_both = lax.optimization_barrier(jnp.concatenate([w_gate, w_up], axis=1))

    experts_range = jnp.arange(EXPERTS, dtype=jnp.int32)
    flat_ids = expert_ids.reshape(tok_rows * 2)
    onehot = (flat_ids[:, None] == experts_range[None, :]).astype(jnp.int32)
    before = jnp.cumsum(onehot, axis=0) - onehot
    target = flat_ids * CAP + jnp.sum(before * onehot, axis=1)
    columns_all = jnp.arange(EXPERTS * CAP, dtype=jnp.int32)
    placement = (
        (target[:, None] == columns_all[None, :]).astype(f32).reshape(tok_rows, 2, EXPERTS * CAP)
    )
    dispatch = jnp.sum(placement, axis=1).astype(bf16)
    down_all = lax.all_gather(w_down, "tp", axis=0)
    context_all = lax.all_gather(context, GROUP, axis=0, tiled=True)
    proj_some = lax.all_gather(out_proj, "a", axis=1, tiled=True)
    proj_some, dispatch, placement, onehot = lax.optimization_barrier(
        (proj_some, dispatch, placement, onehot)
    )
    members = quads * CORES
    head_part = jnp.dot(context_all, proj_some, preferred_element_type=f32).astype(bf16)
    head_part = lax.all_to_all(
        head_part.reshape(members, tok_rows, -1), GROUP, 0, 0, tiled=True
    )
    cols = out_proj.shape[1]
    per = width // cols
    cut = head_part.reshape(members // per, per, tok_rows, EXPERTS, cols)
    cut = jnp.transpose(cut, (3, 0, 2, 1, 4)).reshape(tp, tok_rows, width)
    parts = lax.all_to_all(cut, "tp", 0, 0, tiled=True)
    hstate = (stream.astype(f32) + jnp.sum(parts.astype(f32), axis=0)).astype(bf16)
    hfloat = hstate.astype(f32)
    gain = norm_gain.astype(f32)

    sectioned = lax.dot_general(
        dispatch, hstate, (((0,), (0,)), ((), ())), preferred_element_type=f32
    ).astype(bf16)

    mine = lax.all_to_all(sectioned.reshape(EXPERTS, CAP, width), "a", 0, 0, tiled=True)
    chunk = EXPERTS * CAP
    chip = lax.all_gather(mine.reshape(chunk, width), "q", axis=0, tiled=True)
    other = lax.ppermute(chip, "core", swap)
    first = lax.axis_index("core") == 0
    rows = jnp.concatenate([jnp.where(first, chip, other), jnp.where(first, other, chip)], axis=0)

    rfloat = rows.astype(f32)
    scaled = (rfloat * gain[None, :]).astype(bf16)
    row_sq = jnp.sum(rfloat * rfloat, axis=1)
    both = jnp.dot(scaled, w_both, preferred_element_type=f32).astype(bf16)
    squares = jnp.sum(hfloat * hfloat, axis=1)
    unscaled = jnp.dot(
        hfloat * gain[None, :], router.astype(f32), precision=lax.Precision.HIGHEST
    )
    both, down_all, row_sq, squares, unscaled = lax.optimization_barrier(
        (both, down_all, row_sq, squares, unscaled)
    )
    share = lax.psum_scatter(both, "tp", scatter_dimension=0, tiled=True)
    row_total, total_sq, raw_logits = lax.psum((row_sq, squares, unscaled), "tp")
    my_total = lax.dynamic_slice_in_dim(row_total, lax.axis_index("tp") * chunk, chunk)
    row_inverse = lax.rsqrt(my_total / D + 1e-05)[:, None]
    inverse = lax.rsqrt(total_sq / D + 1e-05)[:, None]
    logits = raw_logits * inverse
    picked = onehot.reshape(tok_rows, 2, EXPERTS).astype(f32)
    chosen = jnp.sum(picked * logits[:, None, :], axis=2)
    leading = jax.nn.sigmoid(chosen[:, 0] - chosen[:, 1])
    weights = jnp.stack([leading, 1.0 - leading], axis=1)
    combine = jnp.sum(placement * weights[:, :, None], axis=1)
    share, row_inverse, combine = lax.optimization_barrier((share, row_inverse, combine))
    ff = w_gate.shape[1]
    wide = share.astype(f32)
    gate_share, up_share = wide[:, :ff] * row_inverse, wide[:, ff:] * row_inverse
    hidden = (jax.nn.silu(gate_share) * up_share).astype(bf16)
    partial_value = jnp.stack(
        [
            jnp.dot(hidden, down_all[f], preferred_element_type=f32).astype(bf16)
            for f in range(tp)
        ]
    )

    halves = partial_value.reshape(CORES, quads, chunk, width)
    from_core = lax.all_to_all(halves, "core", 0, 0, tiled=True)
    on_chip = jnp.sum(from_core.astype(f32), axis=0).astype(bf16)
    from_chips = lax.all_to_all(on_chip, "q", 0, 0, tiled=True)
    summed = jnp.sum(from_chips.astype(f32), axis=0).astype(bf16).reshape(EXPERTS, CAP, width)

    pairs = []
    for q in range(quads):
        for c in range(CORES):
            for t in range(tp):
                dest = flat(tp, t % quads, t // quads, c * quads + q)
                pairs.append((flat(tp, q, c, t), dest))
    turned = lax.ppermute(summed, (*GROUP, "tp"), pairs)
    back = lax.all_to_all(turned, "a", 0, 0, tiled=True)
    expert_mix = jnp.dot(
        combine, back.reshape(chunk, width).astype(f32), precision=lax.Precision.HIGHEST
    )
    return (hfloat + expert_mix).astype(bf16)


def flat(tp, q, core, t):
    return (q * CORES + core) * tp + t


def solution(mesh):
    groups, ep, tp = (mesh.shape[name] for name in ("groups", "ep", "tp"))
    fine = Mesh(
        mesh.devices.reshape(groups, EXPERTS, ep // (EXPERTS * CORES), CORES, tp),
        ("groups", *EP, "tp"),
    )
    rows = ("groups", *EP)
    return jax.shard_map(
        per_device,
        mesh=fine,
        in_specs=(
            P(rows, "tp"),
            P(rows, "tp"),
            P("tp", EP),
            P("tp"),
            P("tp", None),
            P(rows, None),
            P("tp", EP),
            P("tp", EP),
            P(EP, "tp"),
        ),
        out_specs=P(rows, "tp"),
        check_vma=False,
    )
```

```python
import jax
import jax.numpy as jnp
from jax import lax
from jax.experimental import pallas as pl
from jax.experimental.pallas import tpu as pltpu
from jax.sharding import Mesh, PartitionSpec as P

D = 4096
EXPERTS = 4
CAP = 36
CORES = 2
EP = ("a", "q", "core")


def per_device(context, stream, out_proj, norm_gain, router, expert_ids, w_gate, w_up, w_down):
    f32, bf16 = jnp.float32, jnp.bfloat16
    tok_rows, width = stream.shape
    tp = lax.axis_size("tp")
    quads = lax.axis_size("q")
    swap = [(0, 1), (1, 0)]

    w_both = lax.optimization_barrier(jnp.concatenate([w_gate, w_up], axis=1))

    experts_range = jnp.arange(EXPERTS, dtype=jnp.int32)
    flat_ids = expert_ids.reshape(tok_rows * 2)
    onehot = (flat_ids[:, None] == experts_range[None, :]).astype(jnp.int32)
    before = jnp.cumsum(onehot, axis=0) - onehot
    target = flat_ids * CAP + jnp.sum(before * onehot, axis=1)
    columns_all = jnp.arange(EXPERTS * CAP, dtype=jnp.int32)
    placement = (
        (target[:, None] == columns_all[None, :]).astype(f32).reshape(tok_rows, 2, EXPERTS * CAP)
    )
    dispatch = jnp.sum(placement, axis=1).astype(bf16)
    context_all = lax.all_gather(context, "q", axis=0, tiled=True)
    proj_some = lax.all_gather(out_proj, ("a", "core"), axis=1, tiled=True)
    context_all, proj_some, w_down, dispatch, placement, onehot = lax.optimization_barrier(
        (context_all, proj_some, w_down, dispatch, placement, onehot)
    )
    down_all = lax.all_gather(w_down, "tp", axis=0)
    head_part = jnp.dot(context_all, proj_some, preferred_element_type=f32).astype(bf16)
    head_part = lax.all_to_all(head_part.reshape(quads, tok_rows, -1), "q", 0, 0, tiled=True)
    cols = CORES * out_proj.shape[1]
    per = width // cols
    cut = head_part.reshape(quads // per, per, tok_rows, EXPERTS, cols)
    cut = jnp.transpose(cut, (3, 0, 2, 1, 4)).reshape(tp, tok_rows, width)
    parts = lax.all_to_all(cut, "tp", 0, 0, tiled=True)
    hstate = (stream.astype(f32) + jnp.sum(parts.astype(f32), axis=0)).astype(bf16)
    hfloat = hstate.astype(f32)
    gain = norm_gain.astype(f32)

    sectioned = lax.dot_general(
        dispatch, hstate, (((0,), (0,)), ((), ())), preferred_element_type=f32
    ).astype(bf16)

    mine = lax.all_to_all(sectioned.reshape(EXPERTS, CAP, width), "a", 0, 0, tiled=True)
    chunk = EXPERTS * CAP
    chip = lax.all_gather(mine.reshape(chunk, width), "q", axis=0, tiled=True)
    other = lax.ppermute(chip, "core", swap)
    first = lax.axis_index("core") == 0
    rows = jnp.concatenate([jnp.where(first, chip, other), jnp.where(first, other, chip)], axis=0)

    rfloat = rows.astype(f32)
    scaled = (rfloat * gain[None, :]).astype(bf16)
    row_sq = jnp.sum(rfloat * rfloat, axis=1)
    both = jnp.dot(scaled, w_both, preferred_element_type=f32).astype(bf16)
    squares = jnp.sum(hfloat * hfloat, axis=1)
    unscaled = jnp.dot(
        hfloat * gain[None, :], router.astype(f32), precision=lax.Precision.HIGHEST
    )
    both, down_all, row_sq, squares, unscaled = lax.optimization_barrier(
        (both, down_all, row_sq, squares, unscaled)
    )
    share = lax.psum_scatter(both, "tp", scatter_dimension=0, tiled=True)
    row_total, total_sq, raw_logits = lax.psum((row_sq, squares, unscaled), "tp")
    my_total = lax.dynamic_slice_in_dim(row_total, lax.axis_index("tp") * chunk, chunk)
    row_inverse = lax.rsqrt(my_total / D + 1e-05)[:, None]
    inverse = lax.rsqrt(total_sq / D + 1e-05)[:, None]
    logits = raw_logits * inverse
    picked = onehot.reshape(tok_rows, 2, EXPERTS).astype(f32)
    chosen = jnp.sum(picked * logits[:, None, :], axis=2)
    leading = jax.nn.sigmoid(chosen[:, 0] - chosen[:, 1])
    weights = jnp.stack([leading, 1.0 - leading], axis=1)
    combine = jnp.sum(placement * weights[:, :, None], axis=1)
    share, row_inverse, combine = lax.optimization_barrier((share, row_inverse, combine))
    partial_value = down_product(share, row_inverse, down_all)

    halves = partial_value.reshape(CORES, quads, chunk, width)
    from_core = lax.all_to_all(halves, "core", 0, 0, tiled=True)
    on_chip = jnp.sum(from_core.astype(f32), axis=0).astype(bf16)
    from_chips = lax.all_to_all(on_chip, "q", 0, 0, tiled=True)
    summed = jnp.sum(from_chips.astype(f32), axis=0).astype(bf16).reshape(EXPERTS, CAP, width)

    pairs = []
    for q in range(quads):
        for c in range(CORES):
            for t in range(tp):
                dest = flat(tp, t % quads, t // quads, c * quads + q)
                pairs.append((flat(tp, q, c, t), dest))
    turned = lax.ppermute(summed, ("q", "core", "tp"), pairs)
    back = lax.all_to_all(turned, "a", 0, 0, tiled=True)
    expert_mix = jnp.dot(
        combine, back.reshape(chunk, width).astype(f32), precision=lax.Precision.HIGHEST
    )
    return (hfloat + expert_mix).astype(bf16)


def down_body(share_ref, inverse_ref, down_ref, out_ref, hidden_ref):
    ff = hidden_ref.shape[1]

    @pl.when(pl.program_id(0) == 0)
    def _():
        wide = share_ref[...].astype(jnp.float32) * inverse_ref[...]
        gate, up = wide[:, :ff], wide[:, ff:]
        hidden_ref[...] = (jax.nn.silu(gate) * up).astype(jnp.bfloat16)

    out_ref[0] = jnp.dot(
        hidden_ref[...], down_ref[0], preferred_element_type=jnp.float32
    ).astype(jnp.bfloat16)


def down_product(share, inverse, down_all):
    blocks, ff, width = down_all.shape
    rows = share.shape[0]
    return pl.pallas_call(
        down_body,
        grid=(blocks,),
        in_specs=[
            pl.BlockSpec((rows, 2 * ff), lambda i: (0, 0)),
            pl.BlockSpec((rows, 1), lambda i: (0, 0)),
            pl.BlockSpec((1, ff, width), lambda i: (i, 0, 0)),
        ],
        out_specs=pl.BlockSpec((1, rows, width), lambda i: (i, 0, 0)),
        out_shape=jax.ShapeDtypeStruct((blocks, rows, width), jnp.bfloat16),
        scratch_shapes=[pltpu.VMEM((rows, ff), jnp.bfloat16)],
        cost_estimate=pl.CostEstimate(
            flops=2 * blocks * rows * ff * width,
            bytes_accessed=2 * blocks * (ff + rows) * width,
            transcendentals=rows * ff,
        ),
        compiler_params=pltpu.CompilerParams(vmem_limit_bytes=57 * 1024 * 1024),
        name="down",
    )(share, inverse, down_all)


def flat(tp, q, core, t):
    return (q * CORES + core) * tp + t


def solution(mesh):
    groups, ep, tp = (mesh.shape[name] for name in ("groups", "ep", "tp"))
    fine = Mesh(
        mesh.devices.reshape(groups, EXPERTS, ep // (EXPERTS * CORES), CORES, tp),
        ("groups", *EP, "tp"),
    )
    rows = ("groups", *EP)
    return jax.shard_map(
        per_device,
        mesh=fine,
        in_specs=(
            P(rows, "tp"),
            P(rows, "tp"),
            P("tp", EP),
            P("tp"),
            P("tp", None),
            P(rows, None),
            P("tp", EP),
            P("tp", EP),
            P(EP, "tp"),
        ),
        out_specs=P(rows, "tp"),
        check_vma=False,
    )
```

```python
import jax
import jax.numpy as jnp
from jax import lax
from jax.sharding import Mesh, PartitionSpec as P

D = 4096
EXPERTS = 4
CAP = 36
CORES = 2
EP = ("a", "q", "core")


def per_device(context, stream, out_proj, norm_gain, router, expert_ids, w_gate, w_up, w_down):
    f32, bf16 = jnp.float32, jnp.bfloat16
    tok_rows, width = stream.shape
    tp = lax.axis_size("tp")
    quads = lax.axis_size("q")
    swap = [(0, 1), (1, 0)]

    w_both = lax.optimization_barrier(jnp.concatenate([w_gate, w_up], axis=1))

    experts_range = jnp.arange(EXPERTS, dtype=jnp.int32)
    flat_ids = expert_ids.reshape(tok_rows * 2)
    onehot = (flat_ids[:, None] == experts_range[None, :]).astype(jnp.int32)
    before = jnp.cumsum(onehot, axis=0) - onehot
    target = flat_ids * CAP + jnp.sum(before * onehot, axis=1)
    columns_all = jnp.arange(EXPERTS * CAP, dtype=jnp.int32)
    placement = (
        (target[:, None] == columns_all[None, :]).astype(f32).reshape(tok_rows, 2, EXPERTS * CAP)
    )
    dispatch = jnp.sum(placement, axis=1).astype(bf16)
    down_all = lax.all_gather(w_down, "tp", axis=0)
    proj_own = lax.all_gather(out_proj, "a", axis=1, tiled=True)
    context, proj_own, dispatch, placement, onehot = lax.optimization_barrier(
        (context, proj_own, dispatch, placement, onehot)
    )
    proj_other = lax.ppermute(proj_own, "core", swap)
    context_all = lax.all_gather(context, "q", axis=0, tiled=True)
    context_all, proj_other = lax.optimization_barrier((context_all, proj_other))
    first = lax.axis_index("core") == 0
    own, other = (
        jnp.dot(context_all, part, preferred_element_type=f32).astype(bf16)
        for part in (proj_own, proj_other)
    )
    head_part = jnp.concatenate(
        [jnp.where(first, own, other), jnp.where(first, other, own)], axis=1
    )
    head_part = lax.all_to_all(head_part.reshape(quads, tok_rows, -1), "q", 0, 0, tiled=True)
    cols = out_proj.shape[1]
    per = width // (CORES * cols)
    cut = head_part.reshape(quads // per, per, tok_rows, CORES, EXPERTS, cols)
    cut = jnp.transpose(cut, (4, 0, 2, 1, 3, 5)).reshape(tp, tok_rows, width)
    parts = lax.all_to_all(cut, "tp", 0, 0, tiled=True)
    attention = jnp.sum(parts.astype(f32), axis=0)
    hstate = (stream.astype(f32) + attention).astype(bf16)
    hfloat = hstate.astype(f32)
    gain = norm_gain.astype(f32)

    sectioned = lax.dot_general(
        dispatch, hstate, (((0,), (0,)), ((), ())), preferred_element_type=f32
    ).astype(bf16)

    mine = lax.all_to_all(sectioned.reshape(EXPERTS, CAP, width), "a", 0, 0, tiled=True)
    chunk = EXPERTS * CAP
    chip = lax.all_gather(mine.reshape(chunk, width), "q", axis=0, tiled=True)
    other = lax.ppermute(chip, "core", swap)
    rows = jnp.concatenate([jnp.where(first, chip, other), jnp.where(first, other, chip)], axis=0)

    rfloat = rows.astype(f32)
    scaled = (rfloat * gain[None, :]).astype(bf16)
    row_sq = jnp.sum(rfloat * rfloat, axis=1)
    both = jnp.dot(scaled, w_both, preferred_element_type=f32).astype(bf16)
    squares = jnp.sum(hfloat * hfloat, axis=1)
    unscaled = jnp.dot(
        hfloat * gain[None, :], router.astype(f32), precision=lax.Precision.HIGHEST
    )
    both, down_all, row_sq, squares, unscaled = lax.optimization_barrier(
        (both, down_all, row_sq, squares, unscaled)
    )
    share = lax.psum_scatter(both, "tp", scatter_dimension=0, tiled=True)
    row_total, total_sq, raw_logits = lax.psum((row_sq, squares, unscaled), "tp")
    my_total = lax.dynamic_slice_in_dim(row_total, lax.axis_index("tp") * chunk, chunk)
    row_inverse = lax.rsqrt(my_total / D + 1e-05)[:, None]
    inverse = lax.rsqrt(total_sq / D + 1e-05)[:, None]
    logits = raw_logits * inverse
    picked = onehot.reshape(tok_rows, 2, EXPERTS).astype(f32)
    chosen = jnp.sum(picked * logits[:, None, :], axis=2)
    leading = jax.nn.sigmoid(chosen[:, 0] - chosen[:, 1])
    weights = jnp.stack([leading, 1.0 - leading], axis=1)
    combine = jnp.sum(placement * weights[:, :, None], axis=1)
    share, row_inverse, combine = lax.optimization_barrier((share, row_inverse, combine))
    ff = w_gate.shape[1]
    wide = share.astype(f32)
    gate_share, up_share = wide[:, :ff] * row_inverse, wide[:, ff:] * row_inverse
    hidden = (jax.nn.silu(gate_share) * up_share).astype(bf16)
    partial_value = jnp.stack(
        [
            jnp.dot(hidden, down_all[f], preferred_element_type=f32).astype(bf16)
            for f in range(tp)
        ]
    )

    halves = partial_value.reshape(CORES, quads, chunk, width)
    from_core = lax.all_to_all(halves, "core", 0, 0, tiled=True)
    on_chip = jnp.sum(from_core.astype(f32), axis=0).astype(bf16)
    from_chips = lax.all_to_all(on_chip, "q", 0, 0, tiled=True)
    summed = jnp.sum(from_chips.astype(f32), axis=0).astype(bf16).reshape(EXPERTS, CAP, width)

    pairs = []
    for q in range(quads):
        for c in range(CORES):
            for t in range(tp):
                dest = flat(tp, t % quads, t // quads, c * quads + q)
                pairs.append((flat(tp, q, c, t), dest))
    turned = lax.ppermute(summed, ("q", "core", "tp"), pairs)
    back = lax.all_to_all(turned, "a", 0, 0, tiled=True)
    expert_mix = jnp.dot(
        combine, back.reshape(chunk, width).astype(f32), precision=lax.Precision.HIGHEST
    )
    return (hfloat + expert_mix).astype(bf16)


def flat(tp, q, core, t):
    return (q * CORES + core) * tp + t


def solution(mesh):
    groups, ep, tp = (mesh.shape[name] for name in ("groups", "ep", "tp"))
    fine = Mesh(
        mesh.devices.reshape(groups, EXPERTS, ep // (EXPERTS * CORES), CORES, tp),
        ("groups", *EP, "tp"),
    )
    rows = ("groups", *EP)
    return jax.shard_map(
        per_device,
        mesh=fine,
        in_specs=(
            P(rows, "tp"),
            P(rows, "tp"),
            P("tp", EP),
            P("tp"),
            P("tp", None),
            P(rows, None),
            P("tp", EP),
            P("tp", EP),
            P(EP, "tp"),
        ),
        out_specs=P(rows, "tp"),
        check_vma=False,
    )
```

```python
import jax
import jax.numpy as jnp
from jax import lax
from jax.experimental import pallas as pl
from jax.experimental.pallas import tpu as pltpu
from jax.sharding import Mesh, PartitionSpec as P

D = 4096
EXPERTS = 4
CAP = 36
CORES = 2
EP = ("a", "q", "core")


def per_device(context, stream, out_proj, norm_gain, router, expert_ids, w_gate, w_up, w_down):
    f32, bf16 = jnp.float32, jnp.bfloat16
    tok_rows, width = stream.shape
    tp = lax.axis_size("tp")
    quads = lax.axis_size("q")
    swap = [(0, 1), (1, 0)]

    w_both = lax.optimization_barrier(jnp.concatenate([w_gate, w_up], axis=1))

    experts_range = jnp.arange(EXPERTS, dtype=jnp.int32)
    flat_ids = expert_ids.reshape(tok_rows * 2)
    onehot = (flat_ids[:, None] == experts_range[None, :]).astype(jnp.int32)
    before = jnp.cumsum(onehot, axis=0) - onehot
    target = flat_ids * CAP + jnp.sum(before * onehot, axis=1)
    columns_all = jnp.arange(EXPERTS * CAP, dtype=jnp.int32)
    placement = (
        (target[:, None] == columns_all[None, :]).astype(f32).reshape(tok_rows, 2, EXPERTS * CAP)
    )
    dispatch = jnp.sum(placement, axis=1).astype(bf16)
    down_all = lax.all_gather(w_down, "tp", axis=0)
    proj_own = lax.all_gather(out_proj, "a", axis=1, tiled=True)
    proj_own, dispatch, placement, onehot = lax.optimization_barrier(
        (proj_own, dispatch, placement, onehot)
    )
    proj_other = lax.ppermute(proj_own, "core", swap)
    context_all = lax.all_to_all(
        jnp.broadcast_to(context, (quads, *context.shape)), "q", 0, 0, tiled=True
    ).reshape(quads * tok_rows, -1)
    context_all, proj_other = lax.optimization_barrier((context_all, proj_other))
    first = lax.axis_index("core") == 0
    own, other = (
        jnp.dot(context_all, part, preferred_element_type=f32).astype(bf16)
        for part in (proj_own, proj_other)
    )
    head_part = jnp.concatenate(
        [jnp.where(first, own, other), jnp.where(first, other, own)], axis=1
    )
    head_part = lax.all_to_all(head_part.reshape(quads, tok_rows, -1), "q", 0, 0, tiled=True)
    cols = out_proj.shape[1]
    per = width // (CORES * cols)
    cut = head_part.reshape(quads // per, per, tok_rows, CORES, EXPERTS, cols)
    cut = jnp.transpose(cut, (4, 0, 2, 1, 3, 5)).reshape(tp, tok_rows, width)
    parts = lax.all_to_all(cut, "tp", 0, 0, tiled=True)
    attention = jnp.sum(parts.astype(f32), axis=0)
    hstate = (stream.astype(f32) + attention).astype(bf16)
    hfloat = hstate.astype(f32)
    gain = norm_gain.astype(f32)

    sectioned = lax.dot_general(
        dispatch, hstate, (((0,), (0,)), ((), ())), preferred_element_type=f32
    ).astype(bf16)

    mine = lax.all_to_all(sectioned.reshape(EXPERTS, CAP, width), "a", 0, 0, tiled=True)
    chunk = EXPERTS * CAP
    chip = lax.all_gather(mine.reshape(chunk, width), "q", axis=0, tiled=True)
    other = lax.ppermute(chip, "core", swap)
    rows = jnp.concatenate([jnp.where(first, chip, other), jnp.where(first, other, chip)], axis=0)

    rfloat = rows.astype(f32)
    scaled = (rfloat * gain[None, :]).astype(bf16)
    row_sq = jnp.sum(rfloat * rfloat, axis=1)
    both = jnp.dot(scaled, w_both, preferred_element_type=f32).astype(bf16)
    squares = jnp.sum(hfloat * hfloat, axis=1)
    unscaled = jnp.dot(
        hfloat * gain[None, :], router.astype(f32), precision=lax.Precision.HIGHEST
    )
    both, down_all, row_sq, squares, unscaled = lax.optimization_barrier(
        (both, down_all, row_sq, squares, unscaled)
    )
    share = lax.psum_scatter(both, "tp", scatter_dimension=0, tiled=True)
    row_total, total_sq, raw_logits = lax.psum((row_sq, squares, unscaled), "tp")
    my_total = lax.dynamic_slice_in_dim(row_total, lax.axis_index("tp") * chunk, chunk)
    row_inverse = lax.rsqrt(my_total / D + 1e-05)[:, None]
    inverse = lax.rsqrt(total_sq / D + 1e-05)[:, None]
    logits = raw_logits * inverse
    picked = onehot.reshape(tok_rows, 2, EXPERTS).astype(f32)
    chosen = jnp.sum(picked * logits[:, None, :], axis=2)
    leading = jax.nn.sigmoid(chosen[:, 0] - chosen[:, 1])
    weights = jnp.stack([leading, 1.0 - leading], axis=1)
    combine = jnp.sum(placement * weights[:, :, None], axis=1)
    share, row_inverse, combine = lax.optimization_barrier((share, row_inverse, combine))
    partial_value = down_product(share, row_inverse, down_all)

    halves = partial_value.reshape(CORES, quads, chunk, width)
    from_core = lax.all_to_all(halves, "core", 0, 0, tiled=True)
    on_chip = jnp.sum(from_core.astype(f32), axis=0).astype(bf16)
    from_chips = lax.all_to_all(on_chip, "q", 0, 0, tiled=True)
    summed = jnp.sum(from_chips.astype(f32), axis=0).astype(bf16).reshape(EXPERTS, CAP, width)

    pairs = []
    for q in range(quads):
        for c in range(CORES):
            for t in range(tp):
                dest = flat(tp, t % quads, t // quads, c * quads + q)
                pairs.append((flat(tp, q, c, t), dest))
    turned = lax.ppermute(summed, ("q", "core", "tp"), pairs)
    back = lax.all_to_all(turned, "a", 0, 0, tiled=True)
    expert_mix = jnp.dot(
        combine, back.reshape(chunk, width).astype(f32), precision=lax.Precision.HIGHEST
    )
    return (hfloat + expert_mix).astype(bf16)


def down_body(share_ref, inverse_ref, down_ref, out_ref, near_ref, sems):
    blocks, ff, _ = near_ref.shape
    copies = [
        pltpu.make_async_copy(down_ref.at[f], near_ref.at[f], sems.at[f]) for f in range(blocks)
    ]
    for copy in copies:
        copy.start()
    wide = share_ref[...].astype(jnp.float32) * inverse_ref[...]
    hidden = (jax.nn.silu(wide[:, :ff]) * wide[:, ff:]).astype(jnp.bfloat16)
    for f in range(blocks):
        copies[f].wait()
        out_ref[f] = jnp.dot(
            hidden, near_ref[f], preferred_element_type=jnp.float32
        ).astype(jnp.bfloat16)


def down_product(share, inverse, down_all):
    blocks, ff, width = down_all.shape
    rows = share.shape[0]
    near = pl.BlockSpec(memory_space=pltpu.VMEM)
    return pl.pallas_call(
        down_body,
        in_specs=[near, near, pl.BlockSpec(memory_space=pltpu.HBM)],
        out_specs=near,
        out_shape=jax.ShapeDtypeStruct((blocks, rows, width), jnp.bfloat16),
        scratch_shapes=[
            pltpu.VMEM(down_all.shape, jnp.bfloat16),
            pltpu.SemaphoreType.DMA((blocks,)),
        ],
        compiler_params=pltpu.CompilerParams(vmem_limit_bytes=54 * 1024 * 1024),
        cost_estimate=pl.CostEstimate(
            flops=2 * blocks * rows * ff * width,
            bytes_accessed=2 * blocks * (ff + rows) * width,
            transcendentals=rows * ff,
        ),
        name="down",
    )(share, inverse, down_all)


def flat(tp, q, core, t):
    return (q * CORES + core) * tp + t


def solution(mesh):
    groups, ep, tp = (mesh.shape[name] for name in ("groups", "ep", "tp"))
    fine = Mesh(
        mesh.devices.reshape(groups, EXPERTS, ep // (EXPERTS * CORES), CORES, tp),
        ("groups", *EP, "tp"),
    )
    rows = ("groups", *EP)
    return jax.shard_map(
        per_device,
        mesh=fine,
        in_specs=(
            P(rows, "tp"),
            P(rows, "tp"),
            P("tp", EP),
            P("tp"),
            P("tp", None),
            P(rows, None),
            P("tp", EP),
            P("tp", EP),
            P(EP, "tp"),
        ),
        out_specs=P(rows, "tp"),
        check_vma=False,
    )
```

```python
import jax
import jax.numpy as jnp
from jax import lax
from jax.experimental import pallas as pl
from jax.experimental.pallas import tpu as pltpu
from jax.sharding import Mesh, PartitionSpec as P

D = 4096
EXPERTS = 4
CAP = 36
CORES = 2
EP = ("a", "q", "core")


def per_device(context, stream, out_proj, norm_gain, router, expert_ids, w_gate, w_up, w_down):
    f32, bf16 = jnp.float32, jnp.bfloat16
    tok_rows, width = stream.shape
    tp = lax.axis_size("tp")
    quads = lax.axis_size("q")
    swap = [(0, 1), (1, 0)]

    w_both = lax.optimization_barrier(jnp.concatenate([w_gate, w_up], axis=1))

    experts_range = jnp.arange(EXPERTS, dtype=jnp.int32)
    flat_ids = expert_ids.reshape(tok_rows * 2)
    onehot = (flat_ids[:, None] == experts_range[None, :]).astype(jnp.int32)
    before = jnp.cumsum(onehot, axis=0) - onehot
    target = flat_ids * CAP + jnp.sum(before * onehot, axis=1)
    columns_all = jnp.arange(EXPERTS * CAP, dtype=jnp.int32)
    placement = (
        (target[:, None] == columns_all[None, :]).astype(f32).reshape(tok_rows, 2, EXPERTS * CAP)
    )
    dispatch = jnp.sum(placement, axis=1).astype(bf16)
    ff = w_down.shape[0]
    early = (ff // 128 + 1) // 2 * 128
    down_early = lax.all_gather(w_down[:early], "tp", axis=0)
    proj_own = lax.all_gather(out_proj, "a", axis=1, tiled=True)
    proj_own, dispatch, placement, onehot, w_late = lax.optimization_barrier(
        (proj_own, dispatch, placement, onehot, w_down[early:])
    )
    proj_other = lax.ppermute(proj_own, "core", swap)
    context_all = lax.all_to_all(
        jnp.broadcast_to(context, (quads, *context.shape)), "q", 0, 0, tiled=True
    ).reshape(quads * tok_rows, -1)
    context_all, proj_other = lax.optimization_barrier((context_all, proj_other))
    first = lax.axis_index("core") == 0
    own, other = (
        jnp.dot(context_all, part, preferred_element_type=f32).astype(bf16)
        for part in (proj_own, proj_other)
    )
    head_part = jnp.concatenate(
        [jnp.where(first, own, other), jnp.where(first, other, own)], axis=1
    )
    head_part = lax.all_to_all(head_part.reshape(quads, tok_rows, -1), "q", 0, 0, tiled=True)
    cols = out_proj.shape[1]
    per = width // (CORES * cols)
    cut = head_part.reshape(quads // per, per, tok_rows, CORES, EXPERTS, cols)
    cut = jnp.transpose(cut, (4, 0, 2, 1, 3, 5)).reshape(tp, tok_rows, width)
    parts = lax.all_to_all(cut, "tp", 0, 0, tiled=True)
    parts, w_late = lax.optimization_barrier((parts, w_late))
    down_late = lax.all_gather(w_late, "tp", axis=0)
    attention = jnp.sum(parts.astype(f32), axis=0)
    hstate = (stream.astype(f32) + attention).astype(bf16)
    hfloat = hstate.astype(f32)
    gain = norm_gain.astype(f32)

    sectioned = lax.dot_general(
        dispatch, hstate, (((0,), (0,)), ((), ())), preferred_element_type=f32
    ).astype(bf16)

    mine = lax.all_to_all(sectioned.reshape(EXPERTS, CAP, width), "a", 0, 0, tiled=True)
    chunk = EXPERTS * CAP
    chip = lax.all_gather(mine.reshape(chunk, width), "q", axis=0, tiled=True)
    other = lax.ppermute(chip, "core", swap)
    rows = jnp.concatenate([jnp.where(first, chip, other), jnp.where(first, other, chip)], axis=0)

    rfloat = rows.astype(f32)
    scaled = (rfloat * gain[None, :]).astype(bf16)
    row_sq = jnp.sum(rfloat * rfloat, axis=1)
    both = jnp.dot(scaled, w_both, preferred_element_type=f32).astype(bf16)
    squares = jnp.sum(hfloat * hfloat, axis=1)
    unscaled = jnp.dot(
        hfloat * gain[None, :], router.astype(f32), precision=lax.Precision.HIGHEST
    )
    both, down_early, down_late, row_sq, squares, unscaled = lax.optimization_barrier(
        (both, down_early, down_late, row_sq, squares, unscaled)
    )
    share = lax.psum_scatter(both, "tp", scatter_dimension=0, tiled=True)
    row_total, total_sq, raw_logits = lax.psum((row_sq, squares, unscaled), "tp")
    my_total = lax.dynamic_slice_in_dim(row_total, lax.axis_index("tp") * chunk, chunk)
    row_inverse = lax.rsqrt(my_total / D + 1e-05)[:, None]
    inverse = lax.rsqrt(total_sq / D + 1e-05)[:, None]
    logits = raw_logits * inverse
    picked = onehot.reshape(tok_rows, 2, EXPERTS).astype(f32)
    chosen = jnp.sum(picked * logits[:, None, :], axis=2)
    leading = jax.nn.sigmoid(chosen[:, 0] - chosen[:, 1])
    weights = jnp.stack([leading, 1.0 - leading], axis=1)
    combine = jnp.sum(placement * weights[:, :, None], axis=1)
    share, row_inverse, combine = lax.optimization_barrier((share, row_inverse, combine))
    partial_value = down_product(share, row_inverse, down_early, down_late)

    halves = partial_value.reshape(CORES, quads, chunk, width)
    from_core = lax.all_to_all(halves, "core", 0, 0, tiled=True)
    on_chip = jnp.sum(from_core.astype(f32), axis=0).astype(bf16)
    from_chips = lax.all_to_all(on_chip, "q", 0, 0, tiled=True)
    summed = jnp.sum(from_chips.astype(f32), axis=0).astype(bf16).reshape(EXPERTS, CAP, width)

    pairs = []
    for q in range(quads):
        for c in range(CORES):
            for t in range(tp):
                dest = flat(tp, t % quads, t // quads, c * quads + q)
                pairs.append((flat(tp, q, c, t), dest))
    turned = lax.ppermute(summed, ("q", "core", "tp"), pairs)
    back = lax.all_to_all(turned, "a", 0, 0, tiled=True)
    expert_mix = jnp.dot(
        combine, back.reshape(chunk, width).astype(f32), precision=lax.Precision.HIGHEST
    )
    return (hfloat + expert_mix).astype(bf16)


def down_body(share_ref, inverse_ref, early_ref, late_ref, out_ref, near_ref, sems):
    blocks, ff, _ = near_ref.shape
    early = early_ref.shape[1]
    copies = [
        pltpu.make_async_copy(from_ref.at[f], near_ref.at[f, pl.ds(start, size)], sems.at[f, part])
        for f in range(blocks)
        for part, (from_ref, start, size) in enumerate(
            ((early_ref, 0, early), (late_ref, early, ff - early))
        )
    ]
    for copy in copies:
        copy.start()
    wide = share_ref[...].astype(jnp.float32) * inverse_ref[...]
    hidden = (jax.nn.silu(wide[:, :ff]) * wide[:, ff:]).astype(jnp.bfloat16)
    for f in range(blocks):
        copies[2 * f].wait()
        copies[2 * f + 1].wait()
        out_ref[f] = jnp.dot(
            hidden, near_ref[f], preferred_element_type=jnp.float32
        ).astype(jnp.bfloat16)


def down_product(share, inverse, early, late):
    blocks, _, width = early.shape
    ff = early.shape[1] + late.shape[1]
    rows = share.shape[0]
    near = pl.BlockSpec(memory_space=pltpu.VMEM)
    far = pl.BlockSpec(memory_space=pltpu.HBM)
    return pl.pallas_call(
        down_body,
        in_specs=[near, near, far, far],
        out_specs=near,
        out_shape=jax.ShapeDtypeStruct((blocks, rows, width), jnp.bfloat16),
        scratch_shapes=[
            pltpu.VMEM((blocks, ff, width), jnp.bfloat16),
            pltpu.SemaphoreType.DMA((blocks, 2)),
        ],
        compiler_params=pltpu.CompilerParams(vmem_limit_bytes=60 * 1024 * 1024),
        cost_estimate=pl.CostEstimate(
            flops=2 * blocks * rows * ff * width,
            bytes_accessed=2 * blocks * (ff + rows) * width,
            transcendentals=rows * ff,
        ),
        name="down",
    )(share, inverse, early, late)


def flat(tp, q, core, t):
    return (q * CORES + core) * tp + t


def solution(mesh):
    groups, ep, tp = (mesh.shape[name] for name in ("groups", "ep", "tp"))
    fine = Mesh(
        mesh.devices.reshape(groups, EXPERTS, ep // (EXPERTS * CORES), CORES, tp),
        ("groups", *EP, "tp"),
    )
    rows = ("groups", *EP)
    return jax.shard_map(
        per_device,
        mesh=fine,
        in_specs=(
            P(rows, "tp"),
            P(rows, "tp"),
            P("tp", EP),
            P("tp"),
            P("tp", None),
            P(rows, None),
            P("tp", EP),
            P("tp", EP),
            P(EP, "tp"),
        ),
        out_specs=P(rows, "tp"),
        check_vma=False,
    )
```

```python
import jax
import jax.numpy as jnp
from jax import lax
from jax.experimental import pallas as pl
from jax.experimental.pallas import tpu as pltpu
from jax.sharding import Mesh, PartitionSpec as P

D = 4096
EXPERTS = 4
CAP = 36
CORES = 2
EP = ("a", "q", "core")


def per_device(context, stream, out_proj, norm_gain, router, expert_ids, w_gate, w_up, w_down):
    f32, bf16 = jnp.float32, jnp.bfloat16
    tok_rows, width = stream.shape
    tp = lax.axis_size("tp")
    quads = lax.axis_size("q")
    swap = [(0, 1), (1, 0)]

    w_both = lax.optimization_barrier(jnp.concatenate([w_gate, w_up], axis=1))

    experts_range = jnp.arange(EXPERTS, dtype=jnp.int32)
    flat_ids = expert_ids.reshape(tok_rows * 2)
    onehot = (flat_ids[:, None] == experts_range[None, :]).astype(jnp.int32)
    before = jnp.cumsum(onehot, axis=0) - onehot
    target = flat_ids * CAP + jnp.sum(before * onehot, axis=1)
    columns_all = jnp.arange(EXPERTS * CAP, dtype=jnp.int32)
    placement = (
        (target[:, None] == columns_all[None, :]).astype(f32).reshape(tok_rows, 2, EXPERTS * CAP)
    )
    dispatch = jnp.sum(placement, axis=1).astype(bf16)
    ff = w_down.shape[0]
    early = ff - 256
    down_early = lax.all_gather(w_down[:early], "tp", axis=0)
    proj_own = lax.all_gather(out_proj, "a", axis=1, tiled=True)
    proj_own, dispatch, placement, onehot, w_late = lax.optimization_barrier(
        (proj_own, dispatch, placement, onehot, w_down[early:])
    )
    proj_other = lax.ppermute(proj_own, "core", swap)
    context_all = lax.all_to_all(
        jnp.broadcast_to(context, (quads, *context.shape)), "q", 0, 0, tiled=True
    ).reshape(quads * tok_rows, -1)
    context_all, proj_other = lax.optimization_barrier((context_all, proj_other))
    first = lax.axis_index("core") == 0
    own, other = (
        jnp.dot(context_all, part, preferred_element_type=f32).astype(bf16)
        for part in (proj_own, proj_other)
    )
    head_part = jnp.concatenate(
        [jnp.where(first, own, other), jnp.where(first, other, own)], axis=1
    )
    head_part = lax.all_to_all(head_part.reshape(quads, tok_rows, -1), "q", 0, 0, tiled=True)
    cols = out_proj.shape[1]
    per = width // (CORES * cols)
    cut = head_part.reshape(quads // per, per, tok_rows, CORES, EXPERTS, cols)
    cut = jnp.transpose(cut, (4, 0, 2, 1, 3, 5)).reshape(tp, tok_rows, width)
    parts = lax.all_to_all(cut, "tp", 0, 0, tiled=True)
    parts, w_late, down_early = lax.optimization_barrier((parts, w_late, down_early))
    down_late = lax.all_gather(w_late, "tp", axis=0)
    attention = jnp.sum(parts.astype(f32), axis=0)
    hstate = (stream.astype(f32) + attention).astype(bf16)
    hfloat = hstate.astype(f32)
    gain = norm_gain.astype(f32)

    sectioned = lax.dot_general(
        dispatch, hstate, (((0,), (0,)), ((), ())), preferred_element_type=f32
    ).astype(bf16)

    mine = lax.all_to_all(sectioned.reshape(EXPERTS, CAP, width), "a", 0, 0, tiled=True)
    chunk = EXPERTS * CAP
    chip = lax.all_gather(mine.reshape(chunk, width), "q", axis=0, tiled=True)
    other = lax.ppermute(chip, "core", swap)
    rows = jnp.concatenate([jnp.where(first, chip, other), jnp.where(first, other, chip)], axis=0)

    rfloat = rows.astype(f32)
    scaled = (rfloat * gain[None, :]).astype(bf16)
    row_sq = jnp.sum(rfloat * rfloat, axis=1)
    both = jnp.dot(scaled, w_both, preferred_element_type=f32).astype(bf16)
    squares = jnp.sum(hfloat * hfloat, axis=1)
    unscaled = jnp.dot(
        hfloat * gain[None, :], router.astype(f32), precision=lax.Precision.HIGHEST
    )
    both, down_late, row_sq, squares, unscaled = lax.optimization_barrier(
        (both, down_late, row_sq, squares, unscaled)
    )
    share = lax.psum_scatter(both, "tp", scatter_dimension=0, tiled=True)
    row_total, total_sq, raw_logits = lax.psum((row_sq, squares, unscaled), "tp")
    my_total = lax.dynamic_slice_in_dim(row_total, lax.axis_index("tp") * chunk, chunk)
    row_inverse = jnp.broadcast_to(lax.rsqrt(my_total / D + 1e-05)[:, None], (chunk, 128))
    inverse = lax.rsqrt(total_sq / D + 1e-05)[:, None]
    logits = raw_logits * inverse
    picked = onehot.reshape(tok_rows, 2, EXPERTS).astype(f32)
    chosen = jnp.sum(picked * logits[:, None, :], axis=2)
    leading = jax.nn.sigmoid(chosen[:, 0] - chosen[:, 1])
    weights = jnp.stack([leading, 1.0 - leading], axis=1)
    combine = jnp.sum(placement * weights[:, :, None], axis=1)
    share, row_inverse, combine = lax.optimization_barrier((share, row_inverse, combine))
    partial_value = down_product(share, row_inverse, down_early, down_late)

    halves = partial_value.reshape(CORES, quads, chunk, width)
    from_core = lax.all_to_all(halves, "core", 0, 0, tiled=True)
    on_chip = jnp.sum(from_core.astype(f32), axis=0).astype(bf16)
    from_chips = lax.all_to_all(on_chip, "q", 0, 0, tiled=True)
    summed = jnp.sum(from_chips.astype(f32), axis=0).astype(bf16).reshape(EXPERTS, CAP, width)

    pairs = []
    for q in range(quads):
        for c in range(CORES):
            for t in range(tp):
                dest = flat(tp, t % quads, t // quads, c * quads + q)
                pairs.append((flat(tp, q, c, t), dest))
    turned = lax.ppermute(summed, ("q", "core", "tp"), pairs)
    back = lax.all_to_all(turned, "a", 0, 0, tiled=True)
    expert_mix = jnp.dot(
        combine, back.reshape(chunk, width).astype(f32), precision=lax.Precision.HIGHEST
    )
    return (hfloat + expert_mix).astype(bf16)


def down_body(share_ref, inverse_ref, early_ref, late_ref, out_ref, near_ref, sems):
    blocks, ff, _ = near_ref.shape
    early = early_ref.shape[1]
    copies = [
        pltpu.make_async_copy(from_ref.at[f], near_ref.at[f, pl.ds(start, size)], sems.at[f, part])
        for f in range(blocks)
        for part, (from_ref, start, size) in enumerate(
            ((early_ref, 0, early), (late_ref, early, ff - early))
        )
    ]
    for copy in copies:
        copy.start()
    wide = share_ref[...].astype(jnp.float32) * inverse_ref[:, :1]
    hidden = (jax.nn.silu(wide[:, :ff]) * wide[:, ff:]).astype(jnp.bfloat16)
    for f in range(blocks):
        copies[2 * f].wait()
        copies[2 * f + 1].wait()
        out_ref[f] = jnp.dot(
            hidden, near_ref[f], preferred_element_type=jnp.float32
        ).astype(jnp.bfloat16)


def down_product(share, inverse, early, late):
    blocks, _, width = early.shape
    ff = early.shape[1] + late.shape[1]
    rows = share.shape[0]
    near = pl.BlockSpec(memory_space=pltpu.VMEM)
    far = pl.BlockSpec(memory_space=pltpu.HBM)
    return pl.pallas_call(
        down_body,
        in_specs=[near, near, far, far],
        out_specs=near,
        out_shape=jax.ShapeDtypeStruct((blocks, rows, width), jnp.bfloat16),
        scratch_shapes=[
            pltpu.VMEM((blocks, ff, width), jnp.bfloat16),
            pltpu.SemaphoreType.DMA((blocks, 2)),
        ],
        compiler_params=pltpu.CompilerParams(vmem_limit_bytes=60 * 1024 * 1024),
        cost_estimate=pl.CostEstimate(
            flops=2 * blocks * rows * ff * width,
            bytes_accessed=2 * blocks * (ff + rows) * width,
            transcendentals=rows * ff,
        ),
        name="down",
    )(share, inverse, early, late)


def flat(tp, q, core, t):
    return (q * CORES + core) * tp + t


def solution(mesh):
    groups, ep, tp = (mesh.shape[name] for name in ("groups", "ep", "tp"))
    fine = Mesh(
        mesh.devices.reshape(groups, EXPERTS, ep // (EXPERTS * CORES), CORES, tp),
        ("groups", *EP, "tp"),
    )
    rows = ("groups", *EP)
    return jax.shard_map(
        per_device,
        mesh=fine,
        in_specs=(
            P(rows, "tp"),
            P(rows, "tp"),
            P("tp", EP),
            P("tp"),
            P("tp", None),
            P(rows, None),
            P("tp", EP),
            P("tp", EP),
            P(EP, "tp"),
        ),
        out_specs=P(rows, "tp"),
        check_vma=False,
    )
```

```python
import jax
import jax.numpy as jnp
from jax import lax
from jax.experimental import pallas as pl
from jax.experimental.pallas import tpu as pltpu
from jax.sharding import Mesh, PartitionSpec as P

D = 4096
EXPERTS = 4
CAP = 36
CORES = 2
EP = ("a", "q", "core")


def per_device(context, stream, out_proj, norm_gain, router, expert_ids, w_gate, w_up, w_down):
    f32, bf16 = jnp.float32, jnp.bfloat16
    tok_rows, width = stream.shape
    tp = lax.axis_size("tp")
    quads = lax.axis_size("q")
    swap = [(0, 1), (1, 0)]

    w_both = lax.optimization_barrier(jnp.concatenate([w_gate, w_up], axis=1))

    experts_range = jnp.arange(EXPERTS, dtype=jnp.int32)
    flat_ids = expert_ids.reshape(tok_rows * 2)
    onehot = (flat_ids[:, None] == experts_range[None, :]).astype(jnp.int32)
    before = jnp.cumsum(onehot, axis=0) - onehot
    target = flat_ids * CAP + jnp.sum(before * onehot, axis=1)
    columns_all = jnp.arange(EXPERTS * CAP, dtype=jnp.int32)
    placement = (
        (target[:, None] == columns_all[None, :]).astype(f32).reshape(tok_rows, 2, EXPERTS * CAP)
    )
    dispatch = jnp.sum(placement, axis=1).astype(bf16)
    down_all = lax.all_gather(w_down, "tp", axis=0)
    proj_own = lax.all_gather(out_proj, "a", axis=1, tiled=True)
    proj_own, dispatch, placement, onehot = lax.optimization_barrier(
        (proj_own, dispatch, placement, onehot)
    )
    proj_other = lax.ppermute(proj_own, "core", swap)
    context_all = lax.all_to_all(
        jnp.broadcast_to(context, (quads, *context.shape)), "q", 0, 0, tiled=True
    ).reshape(quads * tok_rows, -1)
    context_all, proj_other = lax.optimization_barrier((context_all, proj_other))
    first = lax.axis_index("core") == 0
    own, other = (
        jnp.dot(context_all, part, preferred_element_type=f32).astype(bf16)
        for part in (proj_own, proj_other)
    )
    head_part = jnp.concatenate(
        [jnp.where(first, own, other), jnp.where(first, other, own)], axis=1
    )
    head_part = lax.all_to_all(head_part.reshape(quads, tok_rows, -1), "q", 0, 0, tiled=True)
    cols = out_proj.shape[1]
    per = width // (CORES * cols)
    cut = head_part.reshape(quads // per, per, tok_rows, CORES, EXPERTS, cols)
    cut = jnp.transpose(cut, (4, 0, 2, 1, 3, 5)).reshape(tp, tok_rows, width)
    parts = lax.all_to_all(cut, "tp", 0, 0, tiled=True)
    attention = jnp.sum(parts.astype(f32), axis=0)
    hstate = (stream.astype(f32) + attention).astype(bf16)
    hfloat = hstate.astype(f32)
    gain = norm_gain.astype(f32)

    sectioned = lax.dot_general(
        dispatch, hstate, (((0,), (0,)), ((), ())), preferred_element_type=f32
    ).astype(bf16)

    mine = lax.all_to_all(sectioned.reshape(EXPERTS, CAP, width), "a", 0, 0, tiled=True)
    chunk = EXPERTS * CAP
    chip = lax.all_gather(mine.reshape(chunk, width), "q", axis=0, tiled=True)
    other = lax.ppermute(chip, "core", swap)
    rows = jnp.concatenate([jnp.where(first, chip, other), jnp.where(first, other, chip)], axis=0)

    rfloat = rows.astype(f32)
    scaled = (rfloat * gain[None, :]).astype(bf16)
    row_sq = jnp.sum(rfloat * rfloat, axis=1)
    both = jnp.dot(scaled, w_both, preferred_element_type=f32).astype(bf16)
    squares = jnp.sum(hfloat * hfloat, axis=1)
    unscaled = jnp.dot(
        hfloat * gain[None, :], router.astype(f32), precision=lax.Precision.HIGHEST
    )
    both, down_all, row_sq, squares, unscaled = lax.optimization_barrier(
        (both, down_all, row_sq, squares, unscaled)
    )
    share = lax.psum_scatter(both, "tp", scatter_dimension=0, tiled=True)
    row_total, total_sq, raw_logits = lax.psum((row_sq, squares, unscaled), "tp")
    my_total = lax.dynamic_slice_in_dim(row_total, lax.axis_index("tp") * chunk, chunk)
    row_inverse = lax.rsqrt(my_total / D + 1e-05)[:, None]
    inverse = lax.rsqrt(total_sq / D + 1e-05)[:, None]
    logits = raw_logits * inverse
    picked = onehot.reshape(tok_rows, 2, EXPERTS).astype(f32)
    chosen = jnp.sum(picked * logits[:, None, :], axis=2)
    leading = jax.nn.sigmoid(chosen[:, 0] - chosen[:, 1])
    weights = jnp.stack([leading, 1.0 - leading], axis=1)
    combine = jnp.sum(placement * weights[:, :, None], axis=1)
    share, row_inverse, combine = lax.optimization_barrier((share, row_inverse, combine))
    partial_value = down_product(share, row_inverse, down_all)

    halves = partial_value.reshape(CORES, quads, chunk, width)
    from_core = lax.all_to_all(halves, "core", 0, 0, tiled=True)
    on_chip = jnp.sum(from_core.astype(f32), axis=0).astype(bf16)
    from_chips = lax.all_to_all(on_chip, "q", 0, 0, tiled=True)
    summed = jnp.sum(from_chips.astype(f32), axis=0).astype(bf16).reshape(EXPERTS, CAP, width)

    pairs = []
    for q in range(quads):
        for c in range(CORES):
            for t in range(tp):
                dest = flat(tp, t % quads, t // quads, c * quads + q)
                pairs.append((flat(tp, q, c, t), dest))
    turned = lax.ppermute(summed, ("q", "core", "tp"), pairs)
    back = lax.all_to_all(turned, "a", 0, 0, tiled=True)
    expert_mix = jnp.dot(
        combine, back.reshape(chunk, width).astype(f32), precision=lax.Precision.HIGHEST
    )
    return (hfloat + expert_mix).astype(bf16)


def down_body(share_ref, inverse_ref, down_ref, out_ref, near_ref, sems):
    blocks, ff, _ = near_ref.shape
    copies = [
        pltpu.make_async_copy(down_ref.at[f], near_ref.at[f], sems.at[f]) for f in range(blocks)
    ]
    for copy in copies:
        copy.start()
    wide = share_ref[...].astype(jnp.float32) * inverse_ref[...]
    hidden = (jax.nn.silu(wide[:, :ff]) * wide[:, ff:]).astype(jnp.bfloat16)
    for f in range(blocks):
        copies[f].wait()
        out_ref[f] = jnp.dot(
            hidden, near_ref[f], preferred_element_type=jnp.float32
        ).astype(jnp.bfloat16)


def down_product(share, inverse, down_all):
    blocks, ff, width = down_all.shape
    rows = share.shape[0]
    near = pl.BlockSpec(memory_space=pltpu.VMEM)
    return pl.pallas_call(
        down_body,
        in_specs=[near, near, pl.BlockSpec(memory_space=pltpu.HBM)],
        out_specs=near,
        out_shape=jax.ShapeDtypeStruct((blocks, rows, width), jnp.bfloat16),
        scratch_shapes=[
            pltpu.VMEM(down_all.shape, jnp.bfloat16),
            pltpu.SemaphoreType.DMA((blocks,)),
        ],
        compiler_params=pltpu.CompilerParams(vmem_limit_bytes=50 * 1024 * 1024),
        cost_estimate=pl.CostEstimate(
            flops=2 * blocks * rows * ff * width,
            bytes_accessed=2 * blocks * (ff + rows) * width,
            transcendentals=rows * ff,
        ),
        name="down",
    )(share, inverse, down_all)


def flat(tp, q, core, t):
    return (q * CORES + core) * tp + t


def solution(mesh):
    groups, ep, tp = (mesh.shape[name] for name in ("groups", "ep", "tp"))
    fine = Mesh(
        mesh.devices.reshape(groups, EXPERTS, ep // (EXPERTS * CORES), CORES, tp),
        ("groups", *EP, "tp"),
    )
    rows = ("groups", *EP)
    return jax.shard_map(
        per_device,
        mesh=fine,
        in_specs=(
            P(rows, "tp"),
            P(rows, "tp"),
            P("tp", EP),
            P("tp"),
            P("tp", None),
            P(rows, None),
            P("tp", EP),
            P("tp", EP),
            P(EP, "tp"),
        ),
        out_specs=P(rows, "tp"),
        check_vma=False,
    )
```
